32 devices in a mesh: groups: 2 (over y), tensor: 4 (over z), frames: 4 (over x, core).
Axes of the slice: x: 2, y: 2, z: 4, core: 2. Of those that a mesh axis runs over, the one named last changes fastest.
Arguments:
- patches: bfloat16 [256, 16, 3072], P('tensor', ('groups', 'frames')), parts along dimension 1, may hold values from -12 to 12
- ln_gain: float32 [3072], replicated, may hold values from 0.5 to 1.5
- in_weight: bfloat16 [3072, 4, 768], P('frames', 'tensor'), may hold values from -0.109375 to 0.109375
- q_gain: float32 [4, 128], P('tensor'), may hold values from 0.1 to 1.9
- k_gain: float32 [4, 128], P('tensor'), may hold values from 0.1 to 1.9
- out_weight: bfloat16 [4, 512, 3072], P('tensor', None, 'frames'), may hold values from -0.25 to 0.25
Outputs:
- encoded: bfloat16 [256, 16, 3072], P('tensor', ('groups', 'frames')), parts along dimension 1
The draws below stay inside these ranges and needn't reach their ends.
There are 2 independent parts, one for each index of `groups`. The reference program is written for one: setup_inputs(seed, part) draws one part's arguments, and reference() takes and returns one part's arrays. A program takes and returns all parts, laid end to end along the dimension named above; an argument that names none is the same for every part. Nothing has to cross between parts.
All inputs are finite; a program needn't handle non-finite values.
Results may differ from the reference program's by a relative error of at most 0.022.
Values may be sent and summed in bfloat16 or wider, within the bound.
No kernel may reach another device: no remote copies, remote signals or barrier semaphores. Data moves between devices by JAX's collectives and lax.ppermute only.
A program may use at most 64 MiB of HBM per device.

```python
import math
import jax
import jax.numpy as jnp
from jax import lax

D = 3072
HD = 128
FF_BLOCK = 384
PATCHES = 256
HEADS = 4
FRAMES = 8


def draw_patches(key, part):
    base_key = jax.random.fold_in(key, 7)
    key_base, key_column, key_row = jax.random.split(base_key, 3)
    full_shape = (PATCHES, FRAMES, D)
    base_draw = jax.random.normal(key_base, full_shape, jnp.float32)
    column_scale = jnp.exp(jax.random.uniform(key_column, (D,), jnp.float32, math.log(0.4), math.log(2.5)))
    row_scale = jnp.exp(jax.random.uniform(key_row, (PATCHES, FRAMES, 1), jnp.float32, math.log(0.7), math.log(1.4)))
    return jnp.clip(base_draw * column_scale * row_scale, -12.0, 12.0).astype(jnp.bfloat16)


def steps_of(rng, extent, shards, low, largest):
    level = 1.0
    for position, shards_of in shards:
        draws = jax.random.uniform(jax.random.fold_in(jax.random.fold_in(rng, 6), position), (shards_of,), jnp.float32, low / len(shards), largest / len(shards))
        level = level * jnp.repeat(jnp.exp(draws), extent[position] // shards_of).reshape((-1,) + (1,) * (len(extent) - 1 - position))
    return level


def bell_draw(rng, shape, scale, limit, cuts=(), dtype=jnp.bfloat16):
    gain = steps_of(rng, shape, cuts, -0.22, 0.18) if cuts else 1.0
    values = jax.random.normal(rng, shape, jnp.float32) * scale * gain
    return jnp.minimum(jnp.maximum(values, -limit), limit).astype(dtype)


def setup_inputs(seed: int = 0, part: int = 0) -> dict:
    splits = jax.random.split(jax.random.key(seed), 7)
    part_splits = jax.random.split(jax.random.fold_in(splits[6], part), 7)
    return {
        "patches": draw_patches(jax.random.fold_in(jax.random.fold_in(splits[6], part), 71), part),
        "ln_gain": jnp.clip(1.0 + 0.1 * jax.random.normal(splits[1], (D,), jnp.float32), 0.5, 1.5),
        "in_weight": bell_draw(splits[2], (D, HEADS, 3 * HD + FF_BLOCK), D ** -0.5, 0.109375, ((0, 4), (1, 4))),
        "q_gain": jnp.clip(1.0 + 0.18 * jax.random.normal(splits[3], (HEADS, HD), jnp.float32), 0.1, 1.9),
        "k_gain": jnp.clip(1.0 + 0.18 * jax.random.normal(splits[4], (HEADS, HD), jnp.float32), 0.1, 1.9),
        "out_weight": bell_draw(splits[5], (HEADS, HD + FF_BLOCK, D), (HD + FF_BLOCK) ** -0.5, 0.25, ((0, 4), (2, 4))),
    }


def layer_norm(values, gain_vec):
    mean_val = lax.optimization_barrier(jnp.mean(values, axis=-1, keepdims=True))
    centered = values - mean_val
    variance = lax.optimization_barrier(jnp.mean(centered * centered, axis=-1, keepdims=True))
    return centered * lax.rsqrt(variance + 1e-06) * gain_vec

def reference(patches, ln_gain, in_weight, q_gain, k_gain, out_weight):
    normed = layer_norm(patches.astype(jnp.float32), ln_gain).astype(jnp.bfloat16)
    flat_rows = normed.reshape(PATCHES * FRAMES, D)
    logit_scale = 1.0 / math.sqrt(HD)

    def head_step(running, inputs):
        w_in, gain_q, gain_k, w_out = inputs
        joined_cols = jnp.dot(flat_rows, w_in, preferred_element_type=jnp.float32).reshape(PATCHES, FRAMES, 3 * HD + FF_BLOCK)
        query_slice = layer_norm(joined_cols[..., :HD], gain_q).astype(jnp.bfloat16)
        key_slice = layer_norm(joined_cols[..., HD:2 * HD], gain_k).astype(jnp.bfloat16)
        value_slice = joined_cols[..., 2 * HD:3 * HD].astype(jnp.bfloat16)
        hidden = jax.nn.gelu(joined_cols[..., 3 * HD:], approximate=False).astype(jnp.bfloat16)
        attention_logits = jnp.einsum('ldg,bdg->dlb', query_slice.astype(jnp.float32), key_slice.astype(jnp.float32)) * logit_scale
        exponent_scores = jnp.exp(attention_logits)
        softmax_total = lax.optimization_barrier(jnp.sum(exponent_scores, axis=-1))
        attention_output = jnp.einsum('jdl,ljg->djg', exponent_scores.astype(jnp.bfloat16).astype(jnp.float32), value_slice.astype(jnp.float32))
        attention_output = attention_output / jnp.transpose(softmax_total)[:, :, None]
        blended_rows = jnp.concatenate([attention_output.astype(jnp.bfloat16), hidden], axis=-1).reshape(PATCHES * FRAMES, HD + FF_BLOCK)
        partial_value = jnp.dot(blended_rows, w_out, preferred_element_type=jnp.float32).astype(jnp.bfloat16)
        partial_value = lax.optimization_barrier(partial_value)
        return (running + partial_value.astype(jnp.float32), None)
    in_heads = jnp.transpose(in_weight, (1, 0, 2))
    running, unused = lax.scan(head_step, jnp.zeros((PATCHES * FRAMES, D), jnp.float32), (in_heads, q_gain, k_gain, out_weight))
    return (patches.astype(jnp.float32) + running.reshape(PATCHES, FRAMES, D)).astype(jnp.bfloat16)
```

```python
import functools
import math

import jax
import jax.numpy as jnp
from jax import lax
from jax.sharding import PartitionSpec as P

AXES = ("groups", "tensor", "frames")


def layer_norm(values, gain_vec):
    mean_val = jnp.mean(values, axis=-1, keepdims=True)
    centered = values - mean_val
    variance = jnp.mean(centered * centered, axis=-1, keepdims=True)
    return centered * lax.rsqrt(variance + 1e-06) * gain_vec


def dot(a, b):
    return jnp.dot(a, b, preferred_element_type=jnp.float32)


class Grid:
    def __init__(self, mesh):
        self.G, self.T, self.F = (mesh.shape[a] for a in AXES)
        self.C = 2 if self.F % 2 == 0 else 1
        self.X = self.F // self.C
        self.B = 2 if self.T % 2 == 0 else 1
        self.A = self.T // self.B

    def recv(self, value, dg=0, dq=0, dr=0, dx=0, dc=0):
        G, B, A, X, C = self.G, self.B, self.A, self.X, self.C
        T, F = self.T, self.F
        pairs = []
        for g in range(G):
            for t in range(T):
                for f in range(F):
                    q, r = divmod(t, A)
                    x, c = divmod(f, C)
                    sg = (g + dg) % G
                    st = (q + dq) % B * A + (r + dr) % A
                    sf = (x + dx) % X * C + (c + dc) % C
                    pairs.append(((sg * T + st) * F + sf, (g * T + t) * F + f))
        return lax.ppermute(value, AXES, pairs)


def spread(grid, w_parts):
    G, X, C, B = grid.G, grid.X, grid.C, grid.B
    own = {(0, 0, j): w_parts[j] for j in range(G)}
    mine = w_parts[0]
    other = {}
    if B > 1:
        other[0, 0, 0] = grid.recv(mine, dq=1)
    for i in range(1, X):
        own[i, 0, 0] = grid.recv(mine, dx=i)
    for i in range(1, X):
        if B > 1:
            other[i, 0, 0] = grid.recv(other[0, 0, 0], dx=i)
    for j in range(1, G):
        for i in range(1, X):
            own[i, 0, j] = grid.recv(own[i, 0, 0], dg=j)
        for i in range(X):
            if B > 1:
                other[i, 0, j] = grid.recv(other[i, 0, 0], dg=j)
    for pieces in (own, other):
        for (i, c, j), w in list(pieces.items()):
            for dc in range(1, C):
                pieces[i, dc, j] = grid.recv(w, dc=dc)
    return (own, other)[:B]


def local(grid, patches, ln_gain, in_weight, q_gain, k_gain, out_weight):
    G, A, B, X, C = grid.G, grid.A, grid.B, grid.X, grid.C
    bf16, f32 = jnp.bfloat16, jnp.float32
    rows_p, frames, width = patches.shape
    head_dim = q_gain.shape[1]
    g = lax.axis_index("groups")
    x, c = jnp.divmod(lax.axis_index("frames"), C)
    order = [(i, dc, j) for i in range(X) for dc in range(C) for j in range(G)]

    in_own = in_weight[:, 0, :]
    out_own = out_weight[0]
    part_in = in_own.shape[0] // G
    part_out = out_own.shape[1] // G
    in_parts = [
        lax.dynamic_slice_in_dim(in_own, (g + j) % G * part_in, part_in, 0) for j in range(G)
    ]
    out_parts = [
        lax.dynamic_slice_in_dim(out_own, (g + j) % G * part_out, part_out, 1) for j in range(G)
    ]
    w_in = spread(grid, in_parts)

    def block_of(i, dc, j):
        return ((x + i) % X * C + (c + dc) % C) * G + (g + j) % G

    by_frame = jnp.transpose(patches, (1, 0, 2)).reshape(frames * rows_p, width)
    normed = layer_norm(by_frame.astype(f32), ln_gain).astype(bf16)
    normed = jnp.concatenate(
        [lax.dynamic_slice_in_dim(normed, block_of(*o) * part_in, part_in, 1) for o in order],
        axis=1,
    )
    acts = jnp.concatenate([normed] + [grid.recv(normed, dr=i) for i in range(1, A)], axis=0)
    w_out = spread(grid, out_parts)

    gains = jnp.concatenate([q_gain, k_gain], axis=0)
    gains = (gains, grid.recv(gains, dq=1))[:B]

    rows = A * frames * rows_p
    queries, keys, values, hiddens = [], [], [], []
    for b in range(B):
        joined = jnp.zeros((rows, in_own.shape[1]), f32)
        for n, o in enumerate(order):
            joined = joined + dot(acts[:, n * part_in : (n + 1) * part_in], w_in[b][o])
        queries.append(layer_norm(joined[:, :head_dim], gains[b][0]).astype(bf16))
        keys.append(layer_norm(joined[:, head_dim : 2 * head_dim], gains[b][1]).astype(bf16))
        values.append(joined[:, 2 * head_dim : 3 * head_dim].astype(bf16))
        hiddens.append(jax.nn.gelu(joined[:, 3 * head_dim :], approximate=False).astype(bf16))

    def framed(v):
        v = v.reshape(A, frames, rows_p, head_dim)
        return jnp.transpose(v, (1, 0, 2, 3)).reshape(frames, A * rows_p, head_dim)

    queries = [framed(v) for v in queries]
    keys = [framed(v) for v in keys]
    values = [framed(v) for v in values]
    sets = [[(keys[b], values[b])] for b in range(B)]
    if B > 1:
        both = jnp.stack(keys + values)
        away = grid.recv(both, dq=1)
        for b in range(B):
            sets[b].append((away[1 - b], away[B + 1 - b]))
    blended = []
    for b in range(B):
        total, mixed = 0.0, 0.0
        for key, value in sets[b]:
            logits = jnp.einsum(
                "fqd,fkd->fqk", queries[b], key, preferred_element_type=f32
            ) * (1.0 / math.sqrt(head_dim))
            scores = jnp.exp(logits)
            total = total + jnp.sum(scores, axis=-1, keepdims=True)
            mixed = mixed + jnp.einsum(
                "fqk,fkd->fqd", scores.astype(bf16), value, preferred_element_type=f32
            )
        attended = (mixed / total).astype(bf16).reshape(frames, A, rows_p, head_dim)
        attended = jnp.transpose(attended, (1, 0, 2, 3)).reshape(rows, head_dim)
        blended.append(jnp.concatenate([attended, hiddens[b]], axis=1))

    rows_d = frames * rows_p
    summed = []
    for n in range(X * C):
        cols = []
        for o in order[n * G : (n + 1) * G]:
            acc = dot(blended[0], w_out[0][o])
            for b in range(1, B):
                acc = acc + dot(blended[b], w_out[b][o])
            cols.append(acc)
        acc = jnp.concatenate(cols, axis=1)
        mine = acc[:rows_d]
        for i in range(1, A):
            sent = acc[i * rows_d : (i + 1) * rows_d].astype(bf16)
            mine = mine + grid.recv(sent, dr=-i).astype(f32)
        summed.append(mine)
    summed = jnp.concatenate(summed, axis=1)
    spots = [(s, d, p) for s in range(X) for d in range(C) for p in range(G)]
    natural = []
    for s, d, p in spots:
        at = ((s - x) % X * C + (d - c) % C) * G + (p - g) % G
        natural.append(lax.dynamic_slice_in_dim(summed, at * part_out, part_out, 1))
    natural = jnp.concatenate(natural, axis=1)
    encoded = (by_frame.astype(f32) + natural).astype(bf16)
    return jnp.transpose(encoded.reshape(frames, rows_p, width), (1, 0, 2))


def solution(mesh):
    return jax.shard_map(
        functools.partial(local, Grid(mesh)),
        mesh=mesh,
        in_specs=(
            P("tensor", ("groups", "frames"), None),
            P(),
            P("frames", "tensor", None),
            P("tensor", None),
            P("tensor", None),
            P("tensor", None, "frames"),
        ),
        out_specs=P("tensor", ("groups", "frames"), None),
        check_vma=False,
    )
```
